32 devices in a mesh: dp: 16 (over z, y, x), tp: 2 (over core).
Axes of the slice: x: 2, y: 2, z: 4, core: 2. Of those that a mesh axis runs over, the one named last changes fastest.
Arguments:
- tokens: bfloat16 [2048, 4096], P('dp', 'tp'), may hold values from -6 to 6
- norm_gain: float32 [4096], replicated, may hold values from 0.1 to 1.9
- w_query: bfloat16 [4096, 2048], P(None, 'tp'), may hold values from -0.09375 to 0.09375
- w_key: bfloat16 [4096, 512], P(None, 'tp'), may hold values from -0.09375 to 0.09375
- w_value: bfloat16 [4096, 512], P(None, 'tp'), may hold values from -0.09375 to 0.09375
- w_out: bfloat16 [2048, 4096], P('tp'), may hold values from -0.125 to 0.125
- mlp_gain: float32 [4096], replicated, may hold values from 0.1 to 1.9
- w_gate: bfloat16 [4096, 7168], P(None, 'tp'), may hold values from -0.09375 to 0.09375
- w_up: bfloat16 [4096, 7168], P(None, 'tp'), may hold values from -0.09375 to 0.09375
- w_down: bfloat16 [7168, 4096], P('tp'), may hold values from -0.0625 to 0.0625
- kv_pool: bfloat16 [1024, 2, 4, 128, 128], P('dp', None, 'tp'), may hold values from -160 to 160, as said below
- prefix_len: int32 [16], replicated, may hold values from 1024 to 8192, as said below
- page_owner: int32 [16, 64], replicated, may hold values from -1 to 15, as said below
- page_slot: int32 [16, 64], replicated, may hold values from -1 to 63, as said below
- serving: int32 [16], replicated, may hold values from 0 to 15, each once
Outputs:
- context: bfloat16 [2048, 2048], P('dp', 'tp')
- layer_out: bfloat16 [2048, 4096], P('dp', 'tp')
The draws below stay inside these ranges and needn't reach their ends.
Inputs may be any that keep to these rules, and one draw needn't show every extreme that they name: `prefix_len`: prefix lengths lie between 1024 and 8192; some request has exactly 8192 cached tokens and some exactly 1024. page_owner[r, p] names an index along dp for p < ceil(prefix_len[r] / 128) and is -1 after; no index holds more than 4 pages of one request, and for every request some index holds exactly 4 of its pages. page_slot[r, p] lies in 0 to 63 where page_owner[r, p] is not -1 and is -1 where it is; no two pages share the same holder and slot. serving is a permutation of the requests. `kv_pool`: cached keys and values, each page with an offset of its own.
All inputs are finite; a program needn't handle non-finite values.
Results may differ from the reference program's by a relative error of at most 0.014.
The reference program's roundings to bfloat16 on the way count: a program that leaves them out, or rounds other values in their place, can miss the bound.
Values may be sent and summed in bfloat16 or wider, within the bound.
No kernel may reach another device: no remote copies, remote signals or barrier semaphores. Data moves between devices by JAX's collectives and lax.ppermute only.
A program may use at most 256 MiB of HBM per device.

```python
import math
import jax
import jax.numpy as jnp
from jax import lax

D = 4096
HD = 128
QH = 16
KVH = 4
FF_WIN = 7168
PAGE = 128
MAXP = 64
NEW = 128
REQUESTS = 16
TOKENS = 2048
SLOTS = 1024
PER_OWNER = 4
N_DP = 16
N_TP = 2


def permute_one(sub_key):
    return jax.random.permutation(sub_key, MAXP)


def layout(key):
    shortest = PAGE * MAXP // 8
    longest = PAGE * MAXP
    lengths = jax.random.randint(jax.random.fold_in(key, 101), (REQUESTS,), shortest, longest + 1)
    top_pick = jax.random.randint(jax.random.fold_in(key, 102), (), 0, REQUESTS)
    low_pick = (top_pick + jax.random.randint(jax.random.fold_in(key, 103), (), 1, REQUESTS)) % REQUESTS
    request_ids = jnp.arange(REQUESTS)
    lengths = jnp.where(request_ids == top_pick, longest, jnp.where(request_ids == low_pick, shortest, lengths))
    page_count = (lengths + PAGE - 1) // PAGE
    shifts = jax.random.permutation(jax.random.fold_in(key, 104), REQUESTS)
    relabel = jax.random.permutation(jax.random.fold_in(key, 105), REQUESTS)
    slot_orders = jax.vmap(permute_one)(jax.random.split(jax.random.fold_in(key, 106), REQUESTS))
    page_ids = jnp.arange(MAXP)
    block_ids = page_ids // PER_OWNER
    owner_spot = (block_ids[None, :] + shifts[:, None]) % REQUESTS
    owners = jnp.take(relabel, owner_spot)
    slot_ids = slot_orders[owners, page_ids[None, :]]
    in_prefix = page_ids[None, :] < page_count[:, None]
    return (lengths.astype(jnp.int32), jnp.where(in_prefix, owners, -1).astype(jnp.int32), jnp.where(in_prefix, slot_ids, -1).astype(jnp.int32))


def draw_prefix_len(key, part):
    return layout(key)[0]


def draw_page_owner(key, part):
    return layout(key)[1]


def draw_page_slot(key, part):
    return layout(key)[2]


def draw_kv_pool(key, part):
    base_key = jax.random.fold_in(key, 7)
    page_key = jax.random.fold_in(key, 8)
    full_shape = (SLOTS, 2, KVH, PAGE, HD)
    page_shape = (SLOTS, 2, KVH, 1, HD)
    base = jax.random.normal(base_key, full_shape, jnp.float32)
    offset = jax.random.normal(page_key, page_shape, jnp.float32)
    return (base + offset).astype(jnp.bfloat16)


def steps_of(key, dims, shards, smallest, largest):
    factor_of, own = 1.0, jax.random.fold_in(key, 6)
    for dim, blocks in shards:
        heights = jnp.exp(jax.random.uniform(jax.random.fold_in(own, dim), (blocks,), jnp.float32, smallest / len(shards), largest / len(shards)))
        factor_of = factor_of * jnp.repeat(heights, dims[dim] // blocks).reshape([-1 if axis == dim else 1 for axis in range(len(dims))])
    return factor_of


def normal_values(stream_key, extent, scale, limit, shards=(), held_as=jnp.bfloat16):
    level = steps_of(stream_key, extent, shards, -0.22, 0.18) if shards else 1.0
    entries = jax.random.normal(stream_key, extent, jnp.float32) * scale * level
    return jnp.minimum(jnp.maximum(entries, -limit), limit).astype(held_as)


def setup_inputs(seed: int = 0) -> dict:
    arg_keys = jax.random.split(jax.random.key(seed), 16)
    tokens = normal_values(arg_keys[0], (TOKENS, D), 1.0, 6.0, ((0, 16), (1, 2)))
    norm_gain = jnp.clip(1.0 + 0.18 * jax.random.normal(arg_keys[1], (D,), jnp.float32), 0.1, 1.9)
    w_query = normal_values(arg_keys[2], (D, QH * HD), D ** -0.5, 0.09375, ((1, 2),))
    w_key = normal_values(arg_keys[3], (D, KVH * HD), D ** -0.5, 0.09375, ((1, 2),))
    w_value = normal_values(arg_keys[4], (D, KVH * HD), D ** -0.5, 0.09375, ((1, 2),))
    w_out = normal_values(arg_keys[5], (QH * HD, D), (QH * HD) ** -0.5, 0.125, ((0, 2),))
    mlp_gain = jnp.clip(1.0 + 0.18 * jax.random.normal(arg_keys[6], (D,), jnp.float32), 0.1, 1.9)
    w_gate = normal_values(arg_keys[7], (D, FF_WIN), D ** -0.5, 0.09375, ((1, 2),))
    w_up = normal_values(arg_keys[8], (D, FF_WIN), D ** -0.5, 0.09375, ((1, 2),))
    w_down = normal_values(arg_keys[9], (FF_WIN, D), FF_WIN ** -0.5, 0.0625, ((0, 2),))
    kv_pool = draw_kv_pool(jax.random.fold_in(arg_keys[15], 71), 0)
    prefix_len = draw_prefix_len(jax.random.fold_in(arg_keys[15], 71), 0)
    page_owner = draw_page_owner(jax.random.fold_in(arg_keys[15], 71), 0)
    page_slot = draw_page_slot(jax.random.fold_in(arg_keys[15], 71), 0)
    serving = jax.random.permutation(arg_keys[14], REQUESTS).astype(jnp.int32)
    return {"tokens": tokens, "norm_gain": norm_gain, "w_query": w_query, "w_key": w_key, "w_value": w_value, "w_out": w_out, "mlp_gain": mlp_gain, "w_gate": w_gate, "w_up": w_up, "w_down": w_down, "kv_pool": kv_pool, "prefix_len": prefix_len, "page_owner": page_owner, "page_slot": page_slot, "serving": serving}


EPS = 1e-05
THETA = 500000.0
NEG = -1e+30

def rms_normalize(values, gain):
    as_f32 = values.astype(jnp.float32)
    factor = lax.rsqrt(lax.optimization_barrier(jnp.mean(as_f32 * as_f32, axis=-1, keepdims=True)) + EPS)
    return (as_f32 * factor * gain).astype(jnp.bfloat16)

def rotate(vectors, positions):
    half_dim = vectors.shape[-1] // 2
    freq_index = jnp.arange(half_dim, dtype=jnp.float32)
    inverse = jnp.power(jnp.float32(THETA), -2.0 * freq_index / vectors.shape[-1])
    angles = positions.astype(jnp.float32)[:, None] * inverse[None, :]
    cosine = jnp.cos(angles)[:, None, :]
    sine = jnp.sin(angles)[:, None, :]
    first = vectors[..., :half_dim]
    second = vectors[..., half_dim:]
    return jnp.concatenate([first * cosine - second * sine, second * cosine + first * sine], axis=-1)

def attend(queries, keys_all, values_all, length, new_tokens):
    row_count = queries.shape[1]
    prefix_slots = keys_all.shape[1] - new_tokens
    scores = jnp.einsum('hqd,hkd->hqk', queries.astype(jnp.float32), keys_all.astype(jnp.float32))
    scores = scores / math.sqrt(queries.shape[2])
    row_token = jnp.arange(row_count, dtype=jnp.int32) % new_tokens
    prefix_ok = jnp.arange(prefix_slots, dtype=jnp.int32) < length
    causal = jnp.arange(new_tokens, dtype=jnp.int32)[None, :] <= row_token[:, None]
    allowed = jnp.concatenate([jnp.broadcast_to(prefix_ok[None, :], (row_count, prefix_slots)), causal], axis=1)
    scores = jnp.where(allowed[None], scores, NEG)
    highest = lax.optimization_barrier(jnp.max(scores, axis=-1, keepdims=True))
    expo = jnp.exp(scores - highest)
    weights = (expo / lax.optimization_barrier(jnp.sum(expo, axis=-1, keepdims=True))).astype(jnp.bfloat16)
    result = jnp.einsum('hqk,hkd->hqd', weights.astype(jnp.float32), values_all.astype(jnp.float32))
    return result.astype(jnp.bfloat16)

def rounded_blocks(left, right, blocks):
    block_size = left.shape[1] // blocks
    running = jnp.zeros((left.shape[0], right.shape[1]), jnp.float32)
    for index in range(blocks):
        partial_sum = jnp.dot(left[:, index * block_size:(index + 1) * block_size], right[index * block_size:(index + 1) * block_size], preferred_element_type=jnp.float32)
        partial_sum = lax.optimization_barrier(partial_sum.astype(jnp.bfloat16))
        running = running + partial_sum.astype(jnp.float32)
    return running

def reference(tokens, norm_gain, w_query, w_key, w_value, w_out, mlp_gain, w_gate, w_up, w_down, kv_pool, prefix_len, page_owner, page_slot, serving):
    normed = rms_normalize(tokens, norm_gain)
    starts = jnp.take(prefix_len, serving.astype(jnp.int32))
    positions = (starts[:, None] + jnp.arange(NEW, dtype=jnp.int32)[None, :]).reshape(-1)
    queries = rotate(jnp.dot(normed, w_query, preferred_element_type=jnp.float32).reshape(TOKENS, QH, HD), positions).astype(jnp.bfloat16)
    new_keys = rotate(jnp.dot(normed, w_key, preferred_element_type=jnp.float32).reshape(TOKENS, KVH, HD), positions).astype(jnp.bfloat16)
    new_values = jnp.dot(normed, w_value, preferred_element_type=jnp.float32).astype(jnp.bfloat16).reshape(TOKENS, KVH, HD)
    shared = QH // KVH

    def one_group(items):
        group_q, group_k, group_v, request = items
        length = prefix_len[request]
        owner_row = page_owner[request]
        slot_row = page_slot[request]
        row_index = jnp.where(owner_row >= 0, owner_row * MAXP + slot_row, 0).astype(jnp.int32)
        pages = jnp.take(kv_pool, row_index, axis=0)
        keys_all = jnp.concatenate([pages[:, 0].transpose(1, 0, 2, 3).reshape(KVH, MAXP * PAGE, HD), group_k.transpose(1, 0, 2)], axis=1)
        values_all = jnp.concatenate([pages[:, 1].transpose(1, 0, 2, 3).reshape(KVH, MAXP * PAGE, HD), group_v.transpose(1, 0, 2)], axis=1)
        stacked = group_q.reshape(NEW, KVH, shared, HD).transpose(1, 2, 0, 3).reshape(KVH, shared * NEW, HD)
        result = attend(stacked, keys_all, values_all, length, NEW)
        return result.reshape(KVH, shared, NEW, HD).transpose(2, 0, 1, 3).reshape(NEW, QH * HD)
    context = lax.map(one_group, (queries.reshape(N_DP, NEW, QH, HD), new_keys.reshape(N_DP, NEW, KVH, HD), new_values.reshape(N_DP, NEW, KVH, HD), serving.astype(jnp.int32)))
    context = context.reshape(TOKENS, QH * HD)
    attn_sum = rounded_blocks(context, w_out, N_TP)
    stream = (tokens.astype(jnp.float32) + attn_sum).astype(jnp.bfloat16)
    mlp_in = rms_normalize(stream, mlp_gain)
    gate_act = jnp.dot(mlp_in, w_gate, preferred_element_type=jnp.float32)
    up_act = jnp.dot(mlp_in, w_up, preferred_element_type=jnp.float32)
    hidden = (jax.nn.silu(gate_act) * up_act).astype(jnp.bfloat16)
    mlp_sum = rounded_blocks(hidden, w_down, N_TP)
    layer_out = (stream.astype(jnp.float32) + mlp_sum).astype(jnp.bfloat16)
    return (context, layer_out)
```

```python
import functools
import math

import jax
import jax.numpy as jnp
from jax import lax
from jax.experimental import pallas as pl
from jax.experimental.pallas import tpu as pltpu
from jax.sharding import PartitionSpec as P

EPS = 1e-05
THETA = 500000.0
NEG = -1e30
LOG2E = math.log2(math.e)
MIB = 1024 * 1024


def rotate(vectors, positions):
    half_dim = vectors.shape[-1] // 2
    freq_index = jnp.arange(half_dim, dtype=jnp.float32)
    inverse = jnp.power(jnp.float32(THETA), -2.0 * freq_index / vectors.shape[-1])
    angles = positions.astype(jnp.float32)[:, None] * inverse[None, :]
    cosine = jnp.cos(angles)[:, None, :]
    sine = jnp.sin(angles)[:, None, :]
    first = vectors[..., :half_dim]
    second = vectors[..., half_dim:]
    return jnp.concatenate(
        [first * cosine - second * sine, second * cosine + first * sine], axis=-1
    )


def split(value):
    high = value.astype(jnp.bfloat16)
    low = (value - high.astype(jnp.float32)).astype(jnp.bfloat16)
    return high.astype(jnp.float32), low.astype(jnp.float32)


def put_stats(ref, lead, top, shared, width, pad, stats):
    rows = [s[:, i * width : (i + 1) * width] for s in stats for i in range(shared)]
    if pad > len(rows):
        rows.append(jnp.zeros((pad - len(rows), width), jnp.float32))
    ref[lead + (slice(top, top + pad), slice(None))] = jnp.concatenate(rows, axis=0).astype(
        jnp.bfloat16
    )


def partial_head(scores, values, shared, width, store, stat):
    top = jnp.max(scores, axis=0, keepdims=True)
    high, low = split(top)
    weights = jnp.exp2(scores - (high + low))
    total = jnp.sum(weights, axis=0, keepdims=True)
    sums = lax.dot_general(
        values,
        weights.astype(jnp.bfloat16),
        (((0,), (0,)), ((), ())),
        preferred_element_type=jnp.float32,
    )
    for i in range(shared):
        store(i, sums[:, i * width : (i + 1) * width].astype(jnp.bfloat16))
    stat((high, low) + split(total))


def attend_kernel(count, shared, pad, table, pool, *refs):
    queries = refs[:count]
    outs = refs[count : 2 * count]
    q_buf, page_buf, out_buf, q_sem, page_sem, out_sem = refs[2 * count :]
    per_owner = page_buf.shape[1]
    kv_heads = q_buf.shape[1]
    page_len = page_buf.shape[4]
    head_dim = page_buf.shape[5]
    width = q_buf.shape[3]
    body_rows = shared * head_dim
    scale = LOG2E / math.sqrt(head_dim)

    def page_copy(i, k):
        return pltpu.make_async_copy(
            pool.at[table[i, k]], page_buf.at[i, k], page_sem.at[i, k]
        )

    for i in range(count):
        pltpu.make_async_copy(queries[i], q_buf.at[i], q_sem.at[i]).start()
        for k in range(per_owner):
            page_copy(i, k).start()
    for i in range(count):
        pltpu.make_async_copy(queries[i], q_buf.at[i], q_sem.at[i]).wait()

    def one(i, carry):
        for k in range(per_owner):
            page_copy(i, k).wait()
        any_page = table[i, per_owner]
        for k in range(1, per_owner):
            any_page = any_page + table[i, per_owner + k]

        @pl.when(any_page > 0)
        def _():
            row = lax.broadcasted_iota(jnp.int32, (page_len, width), 0)
            bias = [
                jnp.where(row < table[i, per_owner + k], 0.0, NEG) for k in range(per_owner)
            ]
            bias = jnp.concatenate(bias, axis=0)
            bias = jnp.concatenate([bias] * shared, axis=1)
            for h in range(kv_heads):
                keys = page_buf[i, :, 0, h].reshape(per_owner * page_len, head_dim)
                values = page_buf[i, :, 1, h].reshape(per_owner * page_len, head_dim)
                query = jnp.concatenate(
                    [q_buf[i, h, s * head_dim : (s + 1) * head_dim, :] for s in range(shared)],
                    axis=1,
                )
                scores = jnp.dot(keys, query, preferred_element_type=jnp.float32) * scale + bias

                def store(s, block):
                    out_buf[i, h, s * head_dim : (s + 1) * head_dim, :] = block

                def stat(stats):
                    put_stats(out_buf, (i, h), body_rows, shared, width, pad, stats)

                partial_head(scores, values, shared, width, store, stat)

        @pl.when(any_page == 0)
        def _():
            for h in range(kv_heads):
                out_buf[i, h, 0:body_rows, :] = jnp.zeros((body_rows, width), jnp.bfloat16)
                high, low = split(jnp.full((1, shared * width), NEG, jnp.float32))
                none = jnp.zeros((1, shared * width), jnp.float32)
                put_stats(out_buf, (i, h), body_rows, shared, width, pad, (high, low, none, none))

        return carry

    lax.fori_loop(0, count, one, 0)
    for i in range(count):
        pltpu.make_async_copy(out_buf.at[i], outs[i], out_sem.at[i]).start()
    for i in range(count):
        pltpu.make_async_copy(out_buf.at[i], outs[i], out_sem.at[i]).wait()


def attend_pages(table, pool, queries, pad):
    count = len(queries)
    kv_heads, body_rows, width = queries[0].shape
    head_dim = pool.shape[4]
    shared = body_rows // head_dim
    per_owner = table.shape[1] // 2
    packed = jax.ShapeDtypeStruct((kv_heads, body_rows + pad, width), jnp.bfloat16)
    keys = per_owner * pool.shape[3]
    work = count * kv_heads * keys * shared * width
    return pl.pallas_call(
        functools.partial(attend_kernel, count, shared, pad),
        grid_spec=pltpu.PrefetchScalarGridSpec(
            num_scalar_prefetch=1,
            grid=(),
            in_specs=[pl.BlockSpec(memory_space=pl.ANY)] * (count + 1),
            out_specs=[pl.BlockSpec(memory_space=pl.ANY)] * count,
            scratch_shapes=[
                pltpu.VMEM((count,) + queries[0].shape, jnp.bfloat16),
                pltpu.VMEM((count, per_owner) + pool.shape[1:], jnp.bfloat16),
                pltpu.VMEM((count,) + packed.shape, jnp.bfloat16),
                pltpu.SemaphoreType.DMA((count,)),
                pltpu.SemaphoreType.DMA((count, per_owner)),
                pltpu.SemaphoreType.DMA((count,)),
            ],
        ),
        out_shape=[packed] * count,
        compiler_params=pltpu.CompilerParams(vmem_limit_bytes=24 * MIB),
        cost_estimate=pl.CostEstimate(
            flops=4 * work * head_dim, bytes_accessed=4 * work, transcendentals=work
        ),
        name="attend_pages",
    )(table, pool, *queries)


def attend_new_kernel(shared, pad, query_ref, key_ref, value_ref, out_ref):
    kv_heads, body_rows, width = query_ref.shape
    head_dim = body_rows // shared
    scale = LOG2E / math.sqrt(head_dim)
    row = lax.broadcasted_iota(jnp.int32, (width, width), 0)
    col = lax.broadcasted_iota(jnp.int32, (width, width), 1)
    bias = jnp.where(row <= col, 0.0, NEG)
    bias = jnp.concatenate([bias] * shared, axis=1)
    for h in range(kv_heads):
        keys = key_ref[:, h * head_dim : (h + 1) * head_dim]
        values = value_ref[:, h * head_dim : (h + 1) * head_dim]
        query = jnp.concatenate(
            [query_ref[h, s * head_dim : (s + 1) * head_dim, :] for s in range(shared)], axis=1
        )
        scores = jnp.dot(keys, query, preferred_element_type=jnp.float32) * scale + bias

        def store(s, block):
            out_ref[h, s * head_dim : (s + 1) * head_dim, :] = block

        def stat(stats):
            put_stats(out_ref, (h,), body_rows, shared, width, pad, stats)

        partial_head(scores, values, shared, width, store, stat)


def attend_new(queries, keys, values, shared, pad):
    kv_heads, body_rows, width = queries.shape
    work = kv_heads * width * shared * width
    return pl.pallas_call(
        functools.partial(attend_new_kernel, shared, pad),
        out_shape=jax.ShapeDtypeStruct((kv_heads, body_rows + pad, width), jnp.bfloat16),
        compiler_params=pltpu.CompilerParams(vmem_limit_bytes=8 * MIB),
        cost_estimate=pl.CostEstimate(
            flops=4 * work * body_rows // shared, bytes_accessed=MIB, transcendentals=work
        ),
        name="attend_new",
    )(queries, keys, values)


def weigh(parts, h, body_rows, shared):
    tops, sums = [], []
    for ref in parts:
        stats = ref[h, body_rows : body_rows + 4 * shared, :].astype(jnp.float32)
        tops.append(stats[0:shared] + stats[shared : 2 * shared])
        sums.append(stats[2 * shared : 3 * shared] + stats[3 * shared : 4 * shared])
    top = functools.reduce(jnp.maximum, tops)
    factors = [jnp.exp2(one - top) for one in tops]
    total = functools.reduce(jnp.add, [f * s for f, s in zip(factors, sums)])
    return top, factors, total


def blend(parts, factors, h, s, head_dim):
    terms = [
        ref[h, s * head_dim : (s + 1) * head_dim, :].astype(jnp.float32) * f[s : s + 1, :]
        for ref, f in zip(parts, factors)
    ]
    return functools.reduce(jnp.add, terms)


def merge_kernel(sizes, shared, body_rows, *refs):
    ins, outs = refs[: sum(sizes)], refs[sum(sizes) :]
    head_dim = body_rows // shared
    start = 0
    for size, out in zip(sizes, outs):
        parts = ins[start : start + size]
        start += size
        kv_heads, rows, width = out.shape
        for h in range(kv_heads):
            top, factors, total = weigh(parts, h, body_rows, shared)
            for s in range(shared):
                out[h, s * head_dim : (s + 1) * head_dim, :] = blend(
                    parts, factors, h, s, head_dim
                ).astype(jnp.bfloat16)
            stats = jnp.concatenate(split(top) + split(total), axis=0)
            if rows - body_rows > 4 * shared:
                stats = jnp.concatenate(
                    [stats, jnp.zeros((rows - body_rows - 4 * shared, width), jnp.float32)], axis=0
                )
            out[h, body_rows:rows, :] = stats.astype(jnp.bfloat16)


def merge(groups, shared, body_rows):
    sizes = tuple(len(g) for g in groups)
    flat = [p for g in groups for p in g]
    return pl.pallas_call(
        functools.partial(merge_kernel, sizes, shared, body_rows),
        out_shape=[jax.ShapeDtypeStruct(flat[0].shape, jnp.bfloat16)] * len(groups),
        compiler_params=pltpu.CompilerParams(vmem_limit_bytes=16 * MIB),
        cost_estimate=pl.CostEstimate(
            flops=4 * MIB, bytes_accessed=2 * flat[0].size * (len(flat) + 1), transcendentals=0
        ),
        name="merge",
    )(*flat)


def finish_kernel(count, shared, body_rows, *refs):
    parts, out = refs[:count], refs[count]
    head_dim = body_rows // shared
    for h in range(parts[0].shape[0]):
        _, factors, total = weigh(parts, h, body_rows, shared)
        factors = [f / total for f in factors]
        for s in range(shared):
            col = (h * shared + s) * head_dim
            out[:, col : col + head_dim] = blend(parts, factors, h, s, head_dim).T.astype(
                jnp.bfloat16
            )


def finish(parts, shared, body_rows):
    kv_heads, _, width = parts[0].shape
    return pl.pallas_call(
        functools.partial(finish_kernel, len(parts), shared, body_rows),
        out_shape=jax.ShapeDtypeStruct((width, kv_heads * body_rows), jnp.bfloat16),
        compiler_params=pltpu.CompilerParams(vmem_limit_bytes=16 * MIB),
        cost_estimate=pl.CostEstimate(
            flops=8 * MIB, bytes_accessed=2 * parts[0].size * (len(parts) + 1), transcendentals=0
        ),
        name="finish",
    )(*parts)


class Box:
    def __init__(self, groups):
        self.groups = groups
        self.near = 2 if groups % 2 == 0 else 1
        self.mid = 2 if groups % 4 == 0 else 1
        self.far = groups // (self.near * self.mid)

    def index(self, far, mid, near):
        return ((far % self.far) * self.mid + mid % self.mid) * self.near + near % self.near

    def coords(self, index):
        return index // (self.mid * self.near), index // self.near % self.mid, index % self.near

    def shift(self, array, far, mid, near):
        pairs = []
        for source in range(self.groups):
            a, b, c = self.coords(source)
            pairs.append((source, self.index(a + far, b + mid, c + near)))
        return lax.ppermute(array, "dp", pairs)


def swap_tp(array):
    return lax.ppermute(array, "tp", [(0, 1), (1, 0)])


def gather_tp(own, rank, ranks):
    if ranks != 2:
        return lax.all_gather(own, "tp", axis=1, tiled=True)
    other = swap_tp(own)
    return jnp.where(
        rank == 0,
        jnp.concatenate([own, other], axis=1),
        jnp.concatenate([other, own], axis=1),
    )


def shards(
    tokens,
    norm_gain,
    w_query,
    w_key,
    w_value,
    w_out,
    mlp_gain,
    w_gate,
    w_up,
    w_down,
    kv_pool,
    prefix_len,
    page_owner,
    page_slot,
    serving,
):
    groups = lax.axis_size("dp")
    ranks = lax.axis_size("tp")
    device = lax.axis_index("dp")
    rank = lax.axis_index("tp")
    box = Box(groups)
    new_tokens, share_width = tokens.shape
    model_width = mlp_gain.shape[0]
    pages_max = page_owner.shape[1]
    per_owner = (pages_max + groups - 1) // groups
    page_len = kv_pool.shape[3]
    head_dim = kv_pool.shape[4]
    kv_heads = kv_pool.shape[2]
    q_heads = w_query.shape[1] // head_dim
    shared = q_heads // kv_heads
    body_rows = shared * head_dim
    pad = (4 * shared + 15) // 16 * 16
    group_ids = jnp.arange(groups, dtype=jnp.int32)
    request = jnp.sum(jnp.where(group_ids == device, serving, 0))
    length = jnp.sum(jnp.where(group_ids == request, prefix_len, 0))

    gathered = gather_tp(tokens, rank, ranks)
    gathered_f32 = gathered.astype(jnp.float32)
    in_scale = lax.rsqrt(jnp.mean(gathered_f32 * gathered_f32, axis=-1, keepdims=True) + EPS)
    normed = (gathered_f32 * in_scale * norm_gain).astype(jnp.bfloat16)
    positions = length + jnp.arange(new_tokens, dtype=jnp.int32)
    queries = rotate(
        jnp.dot(normed, w_query, preferred_element_type=jnp.float32).reshape(
            new_tokens, q_heads, head_dim
        ),
        positions,
    ).astype(jnp.bfloat16)
    queries = queries.reshape(new_tokens, q_heads * head_dim).T.reshape(
        kv_heads, body_rows, new_tokens
    )
    new_keys = (
        rotate(
            jnp.dot(normed, w_key, preferred_element_type=jnp.float32).reshape(
                new_tokens, kv_heads, head_dim
            ),
            positions,
        )
        .astype(jnp.bfloat16)
        .reshape(new_tokens, kv_heads * head_dim)
    )
    new_values = jnp.dot(normed, w_value, preferred_element_type=jnp.float32).astype(jnp.bfloat16)

    rows = jnp.take(page_owner, serving, axis=0)
    slots = jnp.take(page_slot, serving, axis=0)
    lengths = jnp.take(prefix_len, serving, axis=0)
    owned = rows == device
    page_ids = jnp.arange(pages_max, dtype=jnp.int32)
    earlier = page_ids[None, :] < page_ids[:, None]
    order = jnp.sum((owned[:, None, :] & earlier[None]).astype(jnp.int32), axis=2)
    choose = jnp.arange(per_owner, dtype=jnp.int32)
    picked = owned[:, None, :] & (order[:, None, :] == choose[None, :, None])
    slot_pick = jnp.sum(jnp.where(picked, slots[:, None, :], 0), axis=2)
    filled = jnp.clip(lengths[:, None] - page_ids[None, :] * page_len, 0, page_len)
    fill_pick = jnp.sum(jnp.where(picked, filled[:, None, :], 0), axis=2)
    tables = jnp.concatenate([slot_pick, fill_pick], axis=1)
    here = box.coords(device)

    own_part = attend_new(queries, new_keys, new_values, shared, pad)
    total_parts = [own_part]
    for far in range(box.far):
        base = queries if far == 0 else box.shift(queries, far, 0, 0)
        offsets, blocks = [(0, 0)], [base]
        for mid in range(box.mid):
            for near in range(box.near):
                if mid and near:
                    continue
                if mid or near:
                    offsets.append((mid, near))
                    blocks.append(box.shift(base, 0, mid, near))
        corner = box.mid == 2 and box.near == 2
        by_near = far % 2 == 0
        if corner:
            offsets.append((1, 1))
            at_near = blocks[offsets.index((0, 1))]
            at_mid = blocks[offsets.index((1, 0))]
            blocks.append(
                box.shift(at_near, 0, 1, 0) if by_near else box.shift(at_mid, 0, 0, 1)
            )
        origin = jnp.stack(
            [box.index(here[0] - far, here[1] - m, here[2] - n) for m, n in offsets]
        )
        table = jnp.take(tables, origin, axis=0)
        parts = attend_pages(table, kv_pool, blocks, pad)
        parts = dict(zip(offsets, parts))
        if corner:
            if by_near:
                back = box.shift(parts[1, 1], 0, -1, 0)
                parts[0, 1] = merge([[parts[0, 1], back]], shared, body_rows)[0]
            else:
                back = box.shift(parts[1, 1], 0, 0, -1)
                parts[1, 0] = merge([[parts[1, 0], back]], shared, body_rows)[0]
        terms = [parts[0, 0]]
        if box.near == 2:
            terms.append(box.shift(parts[0, 1], 0, 0, -1))
        if box.mid == 2:
            terms.append(box.shift(parts[1, 0], 0, -1, 0))
        if far == 0:
            total_parts += terms
        else:
            if len(terms) > 1:
                terms = merge([terms], shared, body_rows)
            total_parts.append(box.shift(terms[0], -far, 0, 0))
    context = finish(total_parts, shared, body_rows)

    projected = jnp.dot(context, w_out, preferred_element_type=jnp.float32).astype(jnp.bfloat16)
    if ranks == 2:
        attn_sum = projected.astype(jnp.float32) + swap_tp(projected).astype(jnp.float32)
    else:
        attn_sum = lax.psum(projected.astype(jnp.float32), "tp")
    stream = (gathered_f32 + attn_sum).astype(jnp.bfloat16)
    stream_f32 = stream.astype(jnp.float32)
    mid_scale = lax.rsqrt(jnp.mean(stream_f32 * stream_f32, axis=-1, keepdims=True) + EPS)
    mlp_in = (stream_f32 * mid_scale * mlp_gain).astype(jnp.bfloat16)
    gate_act = jnp.dot(mlp_in, w_gate, preferred_element_type=jnp.float32)
    up_act = jnp.dot(mlp_in, w_up, preferred_element_type=jnp.float32)
    hidden = (jax.nn.silu(gate_act) * up_act).astype(jnp.bfloat16)
    down_part = jnp.dot(hidden, w_down, preferred_element_type=jnp.float32).astype(jnp.bfloat16)
    stream_own = lax.dynamic_slice_in_dim(stream, rank * share_width, share_width, 1)
    if ranks == 2:
        mine = lax.dynamic_slice_in_dim(down_part, rank * share_width, share_width, 1)
        theirs = lax.dynamic_slice_in_dim(down_part, (1 - rank) * share_width, share_width, 1)
        mlp_own = mine.astype(jnp.float32) + swap_tp(theirs).astype(jnp.float32)
    else:
        mlp_own = lax.psum_scatter(
            down_part, "tp", scatter_dimension=1, tiled=True
        ).astype(jnp.float32)
    layer_out = (stream_own.astype(jnp.float32) + mlp_own).astype(jnp.bfloat16)
    return (context, layer_out)


def solution(mesh):
    in_specs = (
        P("dp", "tp"),
        P(),
        P(None, "tp"),
        P(None, "tp"),
        P(None, "tp"),
        P("tp", None),
        P(),
        P(None, "tp"),
        P(None, "tp"),
        P("tp", None),
        P("dp", None, "tp", None, None),
        P(),
        P(),
        P(),
        P(),
    )
    out_specs = (P("dp", "tp"), P("dp", "tp"))
    return jax.shard_map(shards, mesh=mesh, in_specs=in_specs, out_specs=out_specs, check_vma=False)
```
